32 devices in a mesh: expert: 8 (over z, x), dp: 4 (over y, core).
Axes of the slice: x: 2, y: 2, z: 4, core: 2. Of those that a mesh axis runs over, the one named last changes fastest.
Arguments:
- grad_output: bfloat16 [4096, 2048], P(('expert', 'dp')), may hold values from -1.5 to 1.5
- logits: float32 [4096, 8], P(('expert', 'dp')), may hold values from -6 to 6
- chosen: int32 [4096, 8], P(('expert', 'dp')), may hold values from 0 to 31, as said below
- slots: int32 [4096, 8], P(('expert', 'dp')), may hold values from 0 to 40, as said below
- other_scores: float32 [4096, 8], P(('expert', 'dp')), may hold values from -48 to 48
- hidden: bfloat16 [8, 4, 8, 40, 768], P('expert', 'dp'), may hold values from -6 to 6
- down_weight: bfloat16 [8, 768, 2048], P('expert', 'dp'), may hold values from -0.21875 to 0.21875
Outputs:
- grad_hidden: bfloat16 [8, 4, 8, 40, 768], P('expert', 'dp')
- grad_down: float32 [8, 768, 2048], P('expert', 'dp')
- grad_logits: float32 [4096, 8], P(('expert', 'dp'))
The draws below stay inside these ranges and needn't reach their ends.
Inputs may be any that keep to these rules, and one draw needn't show every extreme that they name: `chosen`: each row names 8 different experts. 40 marks a choice with no slot: its expert is 8 or above, or it comes after 40 earlier choices of the same expert among the rows of one device in row-major order. The live choices of one expert on one device hold slots 0, 1, 2, ... in that order. Some expert fills all 40 slots on some device.
All inputs are finite; a program needn't handle non-finite values.
Results may differ from the reference program's by a relative error of at most 0.023.
Values may be sent and summed in bfloat16 or wider, within the bound.
A program may use at most 64 MiB of HBM per device.

```python
import jax
import jax.numpy as jnp
from jax import lax

D = 2048
FF = 768
TOPK = 8
TOK_DEV = 128
EXPERTS = 32
WINDOW = 8
CAP = 40
TOKENS = 4096
N_EXPERT = 8
N_DP = 4


def route_table(key):
    inner_key = jax.random.fold_in(key, 11)
    random_bits = jax.random.randint(inner_key, (TOKENS, EXPERTS), 0, 1 << 20)
    ranking = random_bits * EXPERTS + jnp.arange(EXPERTS, dtype=jnp.int32)[None, :]
    unused, picked = lax.top_k(ranking, TOPK)
    picked = picked.astype(jnp.int32)
    blocks = picked.reshape(TOKENS // TOK_DEV, TOK_DEV * TOPK)
    onehot = (blocks[:, :, None] == jnp.arange(WINDOW, dtype=jnp.int32)[None, None, :]).astype(jnp.int32)
    ranks = jnp.cumsum(onehot, axis=1) - 1
    position = jnp.sum(ranks * onehot, axis=2)
    inside = (blocks < WINDOW) & (position < CAP)
    placed = jnp.where(inside, position, CAP).astype(jnp.int32)
    return (picked, placed.reshape(TOKENS, TOPK))


def draw_chosen(key, part):
    picked, placed = route_table(key)
    return picked


def draw_slots(key, part):
    picked, placed = route_table(key)
    return placed


def block_levels(rng, extent, shards, smallest, top_value):
    def one(dim, shards_of):
        steps = jax.random.uniform(jax.random.fold_in(jax.random.fold_in(rng, 6), dim), (shards_of,), jnp.float32, smallest / len(shards), top_value / len(shards))
        return jnp.repeat(jnp.exp(steps), extent[dim] // shards_of).reshape((-1,) + (1,) * (len(extent) - dim - 1))

    gain = one(*shards[0])
    for cut in shards[1:]:
        gain = gain * one(*cut)
    return gain


def bell_draw(key, shape, width, reach, pieces=(), kind=jnp.bfloat16):
    factor_of = block_levels(key, shape, pieces, -0.22, 0.18) if pieces else 1.0
    values = jax.random.normal(key, shape, jnp.float32) * width * factor_of
    return jnp.minimum(jnp.maximum(values, -reach), reach).astype(kind)


def setup_inputs(seed: int = 0) -> dict:
    streams_of = jax.random.split(jax.random.key(seed), 8)
    return {
        "grad_output": bell_draw(streams_of[0], (TOKENS, D), 0.25, 1.5, ((0, 32),)),
        "logits": bell_draw(streams_of[1], (TOKENS, TOPK), 1.0, 6.0, ((0, 32),), jnp.float32),
        "chosen": draw_chosen(jax.random.fold_in(streams_of[7], 71), 0),
        "slots": draw_slots(jax.random.fold_in(streams_of[7], 71), 0),
        "other_scores": bell_draw(streams_of[4], (TOKENS, TOPK), 8.0, 48.0, ((0, 32),), jnp.float32),
        "hidden": bell_draw(streams_of[5], (WINDOW, N_DP, N_EXPERT, CAP, FF), 1.0, 6.0, ((0, 8), (1, 4))),
        "down_weight": bell_draw(streams_of[6], (WINDOW, FF, D), FF ** -0.5, 0.21875, ((0, 8), (1, 4))),
    }


def reference(grad_output, logits, chosen, slots, other_scores, hidden, down_weight):
    raised = jnp.exp(logits)
    gating = raised / jnp.sum(raised, axis=1, keepdims=True)
    gate_sent = gating.astype(jnp.bfloat16)
    row_index = jnp.arange(TOKENS, dtype=jnp.int32)
    block_index = row_index // TOK_DEV
    source_index = block_index // N_DP
    shard_index = block_index % N_DP
    live_slot = slots < CAP
    slot_count = N_DP * N_EXPERT * CAP
    total_slots = WINDOW * slot_count
    flat_place = ((chosen * N_DP + shard_index[:, None]) * N_EXPERT + source_index[:, None]) * CAP + slots
    flat_place = jnp.where(live_slot, flat_place, total_slots).astype(jnp.int32).reshape(-1)
    pair_index = jnp.arange(TOKENS * TOPK, dtype=jnp.int32)
    owners = jnp.zeros((total_slots + 1,), jnp.int32).at[flat_place].set(pair_index)
    filled = jnp.zeros((total_slots + 1,), jnp.float32).at[flat_place].set(1.0)
    owners = owners[:total_slots].reshape(WINDOW, slot_count)
    filled = filled[:total_slots].reshape(WINDOW, slot_count)
    gate_flat = gate_sent.reshape(-1)

    def expert_pass(inputs):
        owner_rows, fill_rows, expert_hidden, expert_weight = inputs
        slot_mask = fill_rows.astype(jnp.bfloat16)
        slot_rows = grad_output[owner_rows // TOPK] * slot_mask[:, None]
        slot_gate = (gate_flat[owner_rows] * slot_mask).astype(jnp.float32)
        local_hidden = expert_hidden.reshape(slot_count, FF)
        upward = lax.dot_general(slot_rows, expert_weight, (((1,), (1,)), ((), ())), preferred_element_type=jnp.float32)
        grad_rows = (slot_gate[:, None] * upward).astype(jnp.bfloat16)
        outputs = jnp.dot(local_hidden, expert_weight, preferred_element_type=jnp.float32)
        slot_scores = jnp.sum(slot_rows.astype(jnp.float32) * outputs, axis=1)
        scaled = (slot_gate[:, None] * slot_rows.astype(jnp.float32)).astype(jnp.bfloat16)

        def add_shard(totals, shard):
            shard_hidden, shard_scaled = shard
            partial_value = lax.dot_general(shard_hidden, shard_scaled, (((0,), (0,)), ((), ())), preferred_element_type=jnp.float32)
            rounded = lax.optimization_barrier(partial_value.astype(jnp.bfloat16))
            return totals + rounded.astype(jnp.float32), None

        grads, unused = lax.scan(add_shard, jnp.zeros((FF, D), jnp.float32),
                                 (local_hidden.reshape(N_DP, N_EXPERT * CAP, FF), scaled.reshape(N_DP, N_EXPERT * CAP, D)))
        return grad_rows, grads, slot_scores

    grad_rows, grad_down, slot_scores = lax.map(expert_pass, (owners, filled, hidden, down_weight))
    grad_hidden = grad_rows.reshape(WINDOW, N_DP, N_EXPERT, CAP, FF)
    score_flat = jnp.concatenate([slot_scores.reshape(-1), jnp.zeros((1,), jnp.float32)])
    token_scores = score_flat[flat_place].reshape(TOKENS, TOPK)
    outside = jnp.where(chosen >= WINDOW, other_scores, jnp.float32(0.0))
    scores_all = jnp.where(live_slot, token_scores, outside)
    mean_score = jnp.sum(gating * scores_all, axis=1, keepdims=True)
    grad_logits = gating * (scores_all - mean_score)
    return grad_hidden, grad_down, grad_logits
```

```python
import functools

import jax
import jax.numpy as jnp
from jax import lax
from jax.experimental import pallas as pl
from jax.experimental.pallas import tpu as pltpu
from jax.sharding import PartitionSpec as P

MESH = pl.DeviceIdType.MESH
PIECES = 4


def kernel(
    window, shards, capacity, pieces,
    token_ref, meta_ref, hidden_ref, weight_ref,
    gradh_ref, down_ref, logit_ref,
    rsend, rrecv, msend, mrecv, wfull, padded, hturn, upward, own, csend, crecv, ysend, yrecv,
    tsend, trecv, gates,
    rs, rr, ms, mr, ws, wr, fs, fr, cs, cr, ys, yr, ts, tr,
):
    me = lax.axis_index("expert")
    place = lax.axis_index("dp")
    chip, core = place // 2, place % 2
    chips = shards // 2
    mate = (me, chip * 2 + 1 - core)
    tokens, width = token_ref.shape
    piece = width // pieces
    rows = rsend.shape[2]
    slots_all = window * rows
    shard_rows, hidden_units = weight_ref.shape[0], hidden_ref.shape[2]

    def other(step):
        return lax.rem(me + step, window)

    def chip_at(step):
        return lax.rem(chip + step, chips)

    def across(step):
        return (me, chip_at(step) * 2 + core)

    barrier = pltpu.get_barrier_semaphore()
    for step in range(1, window):
        pl.semaphore_signal(barrier, inc=1, device_id=(other(step), place), device_id_type=MESH)
    for step in range(1, chips):
        pl.semaphore_signal(barrier, inc=1, device_id=across(step), device_id_type=MESH)
    pl.semaphore_signal(barrier, inc=1, device_id=mate, device_id_type=MESH)

    k = logit_ref.shape[0]
    raised = jnp.exp(meta_ref[0:k])
    gating = raised / jnp.sum(raised, axis=0, keepdims=True)
    sent_gate = gating.astype(jnp.bfloat16).astype(jnp.float32)
    chosen = meta_ref[k : 2 * k]
    slots = meta_ref[2 * k : 3 * k]
    outside = jnp.where(chosen >= window, meta_ref[3 * k : 4 * k], 0.0)
    live = slots < capacity
    for w in range(window):
        here = live & (chosen == w)
        pos = jnp.sum(jnp.where(here, slots + 1.0, 0.0), axis=0, keepdims=True) - 1.0
        gate = jnp.sum(jnp.where(here, sent_gate, 0.0), axis=0, keepdims=True)
        line = lax.broadcasted_iota(jnp.int32, (8, tokens), 0)
        msend[w] = jnp.where(line == 0, pos, gate)

    slot_id = lax.broadcasted_iota(jnp.int32, (rows, tokens), 0).astype(jnp.float32)

    def spread(ref, w):
        return slot_id == ref[w, 0:1, :]

    dispatch = jnp.concatenate(
        [spread(msend, w).astype(jnp.float32) for w in range(window)], axis=0
    ).astype(jnp.bfloat16)

    def fill(c):
        lanes = pl.ds(pl.multiple_of(c * piece, piece), piece)
        placed = jnp.dot(dispatch, token_ref[:, lanes], preferred_element_type=jnp.float32)
        rsend[c] = placed.astype(jnp.bfloat16).reshape(window, rows, piece)

    def row_copy(c, dest, source):
        return pltpu.make_async_remote_copy(
            src_ref=rsend.at[c, dest, pl.ds(0, capacity)],
            dst_ref=rrecv.at[c, source, pl.ds(0, capacity)],
            send_sem=rs.at[c, dest], recv_sem=rr.at[c, source],
            device_id=(dest, place), device_id_type=MESH,
        )

    def meta_copy(dest, source):
        return pltpu.make_async_remote_copy(
            src_ref=msend.at[dest], dst_ref=mrecv.at[source],
            send_sem=ms.at[dest], recv_sem=mr.at[source],
            device_id=(dest, place), device_id_type=MESH,
        )

    def score_copy(dest, source):
        return pltpu.make_async_remote_copy(
            src_ref=tsend.at[dest], dst_ref=trecv.at[source],
            send_sem=ts.at[dest], recv_sem=tr.at[source],
            device_id=(dest, place), device_id_type=MESH,
        )

    def weight_copy(c, target, step, slot):
        lanes = pl.ds(pl.multiple_of(c * piece, piece), piece)
        return pltpu.make_async_remote_copy(
            src_ref=weight_ref.at[:, lanes], dst_ref=wfull.at[c, slot],
            send_sem=ws.at[c, step], recv_sem=wr.at[c, step],
            device_id=target, device_id_type=MESH,
        )

    def pass_copy(c, step, slot):
        return pltpu.make_async_remote_copy(
            src_ref=wfull.at[c, slot], dst_ref=wfull.at[c, slot],
            send_sem=fs.at[c, step], recv_sem=fr.at[c, step],
            device_id=mate, device_id_type=MESH,
        )

    def core_copy(c):
        return pltpu.make_async_remote_copy(
            src_ref=csend.at[c], dst_ref=crecv.at[c],
            send_sem=cs.at[c], recv_sem=cr.at[c],
            device_id=mate, device_id_type=MESH,
        )

    def sum_copy(c, step):
        return pltpu.make_async_remote_copy(
            src_ref=ysend.at[c, step], dst_ref=yrecv.at[c, step],
            send_sem=ys.at[c, step], recv_sem=yr.at[c, step],
            device_id=across(step), device_id_type=MESH,
        )

    fill(0)
    pl.semaphore_wait(barrier, window - 1 + chips)

    for step in range(1, window):
        meta_copy(other(step), me).start()

    def launch(c, carry):
        for step in range(1, window):
            row_copy(c, other(step), me).start()
        for step in range(1, chips):
            weight_copy(c, across(step), step, place).start()
        weight_copy(c, mate, 0, place).start()

        @pl.when(c + 1 < pieces)
        def _():
            fill(c + 1)

        return carry

    lax.fori_loop(0, pieces, launch, 0)

    mrecv[me] = msend[me]
    for c in range(pieces):
        lanes = slice(c * piece, (c + 1) * piece)
        rrecv[c, me, 0:capacity] = rsend[c, me, 0:capacity]
        if rows > capacity:
            rrecv[c, :, capacity:rows] = jnp.zeros((window, rows - capacity, piece), jnp.bfloat16)
        wfull[c, place] = weight_ref[:, lanes]
    padded[:, 0:capacity] = hidden_ref[...]
    if rows > capacity:
        padded[:, capacity:rows] = jnp.zeros((window, rows - capacity, hidden_units), jnp.bfloat16)
    flat = padded[...].reshape(slots_all, hidden_units)
    hturn[...] = flat.T.reshape(shards, shard_rows, slots_all)
    upward[...] = jnp.zeros_like(upward)

    for step in range(1, window):
        meta_copy(other(step), lax.rem(me + window - step, window)).wait_recv()
    for s in range(window):
        gates[s] = jnp.sum(
            jnp.where(spread(mrecv, s), mrecv[s, 1:2, :], 0.0), axis=1, keepdims=True
        )

    def finish(c, carry):
        lanes = pl.ds(pl.multiple_of(c * piece, piece), piece)
        for step in range(1, chips):
            came = lax.rem(chip + chips - step, chips) * 2 + core
            weight_copy(c, across(step), step, came).wait_recv()
            pass_copy(c, step, came).start()
        for step in range(1, window):
            row_copy(c, other(step), lax.rem(me + window - step, window)).wait_recv()
        got = rrecv[c].reshape(slots_all, piece)
        scaled = (gates[...].reshape(slots_all, 1) * got.astype(jnp.float32)).astype(jnp.bfloat16)
        for h in range(chips):
            csend[c, h] = jnp.dot(
                hturn[2 * h + 1 - core], scaled, preferred_element_type=jnp.float32
            ).astype(jnp.bfloat16)
        core_copy(c).start()
        for h in range(chips):
            own[h] = jnp.dot(hturn[2 * h + core], scaled, preferred_element_type=jnp.float32)
        core_copy(c).wait_recv()
        for step in range(1, chips):
            to = chip_at(step)
            ysend[c, step] = (own[to] + crecv[c, to].astype(jnp.float32)).astype(jnp.bfloat16)
            sum_copy(c, step).start()
        down_ref[:, lanes] = own[chip] + crecv[c, chip].astype(jnp.float32)
        weight_copy(c, mate, 0, chip * 2 + 1 - core).wait_recv()
        for step in range(1, chips):
            came = lax.rem(chip + chips - step, chips) * 2 + 1 - core
            pass_copy(c, step, came).wait_recv()
        weights = wfull[c].reshape(hidden_units, piece)
        upward[...] += lax.dot_general(
            got, weights, (((1,), (1,)), ((), ())), preferred_element_type=jnp.float32
        )
        return carry

    lax.fori_loop(0, pieces, finish, 0)

    for s in range(window):
        up = upward[s * rows : (s + 1) * rows]
        score = jnp.sum(padded[s].astype(jnp.float32) * up, axis=1, keepdims=True)
        back = jnp.sum(jnp.where(spread(mrecv, s), score, 0.0), axis=0, keepdims=True)
        tsend[s] = jnp.broadcast_to(back, (8, tokens))
    for step in range(1, window):
        score_copy(other(step), me).start()
    trecv[me] = tsend[me]
    for s in range(window):
        up = upward[s * rows : s * rows + capacity]
        gradh_ref[s] = (gates[s, 0:capacity] * up).astype(jnp.bfloat16)

    for step in range(1, window):
        score_copy(other(step), lax.rem(me + window - step, window)).wait_recv()
    token_scores = jnp.zeros((k, tokens), jnp.float32)
    for w in range(window):
        token_scores = jnp.where(chosen == w, trecv[w], token_scores)
    scores_all = jnp.where(live, token_scores, outside)
    mean_score = jnp.sum(gating * scores_all, axis=0, keepdims=True)
    logit_ref[...] = gating * (scores_all - mean_score)

    def collect(c, carry):
        lanes = pl.ds(pl.multiple_of(c * piece, piece), piece)
        for step in range(1, chips):
            sum_copy(c, step).wait_recv()
            down_ref[:, lanes] += yrecv[c, step].astype(jnp.float32)
        return carry

    lax.fori_loop(0, pieces, collect, 0)

    def drain(c, carry):
        for step in range(1, window):
            row_copy(c, other(step), me).wait_send()
        for step in range(1, chips):
            weight_copy(c, across(step), step, place).wait_send()
            pass_copy(c, step, lax.rem(chip + chips - step, chips) * 2 + core).wait_send()
            sum_copy(c, step).wait_send()
        weight_copy(c, mate, 0, place).wait_send()
        core_copy(c).wait_send()
        return carry

    lax.fori_loop(0, pieces, drain, 0)
    for step in range(1, window):
        meta_copy(other(step), me).wait_send()
        score_copy(other(step), me).wait_send()


def fused(grad_output, logits, chosen, slots, other_scores, hidden, down_weight):
    window = lax.axis_size("expert")
    shards = lax.axis_size("dp")
    capacity, hidden_units = hidden.shape[3], hidden.shape[4]
    tokens, width = grad_output.shape
    k = logits.shape[1]
    shard_rows = down_weight.shape[1]
    rows = -(-capacity // 16) * 16
    chips = shards // 2
    piece = width // PIECES
    meta = jnp.concatenate(
        [logits, chosen.astype(jnp.float32), slots.astype(jnp.float32), other_scores], axis=1
    ).T
    vmem = pl.BlockSpec(memory_space=pltpu.VMEM)
    bf, f32, dma = jnp.bfloat16, jnp.float32, pltpu.SemaphoreType.DMA
    slots_all = window * rows
    gradh, down, turned = pl.pallas_call(
        functools.partial(kernel, window, shards, capacity, PIECES),
        out_shape=(
            jax.ShapeDtypeStruct((window, capacity, hidden_units), bf),
            jax.ShapeDtypeStruct((shard_rows, width), f32),
            jax.ShapeDtypeStruct((k, tokens), f32),
        ),
        in_specs=[vmem] * 4,
        out_specs=(vmem,) * 3,
        scratch_shapes=[
            pltpu.VMEM((PIECES, window, rows, piece), bf),
            pltpu.VMEM((PIECES, window, rows, piece), bf),
            pltpu.VMEM((window, 8, tokens), f32),
            pltpu.VMEM((window, 8, tokens), f32),
            pltpu.VMEM((PIECES, shards, shard_rows, piece), bf),
            pltpu.VMEM((window, rows, hidden_units), bf),
            pltpu.VMEM((shards, shard_rows, slots_all), bf),
            pltpu.VMEM((slots_all, hidden_units), f32),
            pltpu.VMEM((chips, shard_rows, piece), f32),
            pltpu.VMEM((PIECES, chips, shard_rows, piece), bf),
            pltpu.VMEM((PIECES, chips, shard_rows, piece), bf),
            pltpu.VMEM((PIECES, chips, shard_rows, piece), bf),
            pltpu.VMEM((PIECES, chips, shard_rows, piece), bf),
            pltpu.VMEM((window, 8, tokens), f32),
            pltpu.VMEM((window, 8, tokens), f32),
            pltpu.VMEM((window, rows, 1), f32),
            dma((PIECES, window)), dma((PIECES, window)),
            dma((window,)), dma((window,)),
            dma((PIECES, chips)), dma((PIECES, chips)),
            dma((PIECES, chips)), dma((PIECES, chips)),
            dma((PIECES,)), dma((PIECES,)),
            dma((PIECES, chips)), dma((PIECES, chips)),
            dma((window,)), dma((window,)),
        ],
        compiler_params=pltpu.CompilerParams(
            collective_id=0, has_side_effects=True, vmem_limit_bytes=48 * 1024 * 1024
        ),
    )(grad_output, meta, hidden.reshape(window, capacity, hidden_units), down_weight.reshape(shard_rows, width))
    return (gradh.reshape(hidden.shape), down.reshape(1, shard_rows, width), turned.T)


def plain(grad_output, logits, chosen, slots, other_scores, hidden, down_weight):
    window = lax.axis_size("expert")
    capacity = hidden.shape[3]
    hidden_units = hidden.shape[4]
    model_width = grad_output.shape[1]
    shard_rows = down_weight.shape[1]
    raised = jnp.exp(logits)
    gating = raised / jnp.sum(raised, axis=1, keepdims=True)
    gate_sent = gating.astype(jnp.bfloat16)
    live_slot = slots < capacity
    target = jnp.where(live_slot, chosen * capacity + slots, window * capacity)
    columns = jnp.arange(window * capacity, dtype=jnp.int32)
    placing = (target[:, :, None] == columns[None, None, :]).astype(jnp.bfloat16)
    dispatch = jnp.sum(placing, axis=1)
    send_rows = jnp.einsum(
        "tr,td->rd", dispatch, grad_output, preferred_element_type=jnp.float32
    ).astype(jnp.bfloat16)
    send_gate = jnp.einsum(
        "tkr,tk->r", placing, gate_sent, preferred_element_type=jnp.float32
    ).astype(jnp.bfloat16)
    placing_float = placing.astype(jnp.float32)
    send_rows = send_rows.reshape(window, capacity, model_width)
    send_gate = send_gate.reshape(window, capacity)
    recv_rows, recv_gate = (
        lax.all_to_all(send_rows, "expert", split_axis=0, concat_axis=0, tiled=True),
        lax.all_to_all(send_gate, "expert", split_axis=0, concat_axis=0, tiled=True),
    )
    slot_rows = recv_rows.reshape(-1, model_width)
    slot_gate = recv_gate.reshape(-1).astype(jnp.float32)
    local_hidden = hidden.reshape(-1, hidden_units)
    scaled = (slot_gate[:, None] * slot_rows.astype(jnp.float32)).astype(jnp.bfloat16)
    weights = down_weight.reshape(shard_rows, model_width)
    product = lax.dot_general(
        slot_rows,
        lax.all_gather(weights, "dp", axis=0, tiled=True),
        (((1,), (1,)), ((), ())),
        preferred_element_type=jnp.float32,
    )
    grad_rows = lax.psum_scatter(
        lax.dot_general(
            local_hidden, scaled, (((0,), (0,)), ((), ())), preferred_element_type=jnp.float32
        ).astype(jnp.bfloat16),
        "dp",
        scatter_dimension=0,
        tiled=True,
    ).astype(jnp.float32)
    slot_scores = jnp.sum(local_hidden.astype(jnp.float32) * product, axis=1)
    grad_hidden = (slot_gate[:, None] * product).astype(jnp.bfloat16).reshape(hidden.shape)
    returned = lax.all_to_all(
        slot_scores.reshape(window, capacity), "expert", split_axis=0, concat_axis=0, tiled=True
    )
    token_scores = jnp.einsum(
        "tkr,r->tk", placing_float, returned.reshape(-1), precision=lax.Precision.HIGHEST
    )
    outside = jnp.where(chosen >= window, other_scores, jnp.float32(0.0))
    scores_all = jnp.where(live_slot, token_scores, outside)
    mean_score = jnp.sum(gating * scores_all, axis=1, keepdims=True)
    grad_logits = gating * (scores_all - mean_score)
    return (grad_hidden, grad_rows.reshape(1, shard_rows, model_width), grad_logits)


def body(grad_output, logits, chosen, slots, other_scores, hidden, down_weight):
    args = (grad_output, logits, chosen, slots, other_scores, hidden, down_weight)
    fits = (
        lax.axis_size("dp") % 2 == 0
        and hidden.shape[3] % 8 == 0
        and down_weight.shape[1] % 16 == 0
        and hidden.shape[4] % 128 == 0
        and grad_output.shape[0] == 128
        and grad_output.shape[1] % (PIECES * 128) == 0
        and logits.shape[1] == 8
    )
    return fused(*args) if fits else plain(*args)


def solution(mesh):
    placed = (
        P(("expert", "dp"), None),
        P(("expert", "dp"), None),
        P(("expert", "dp"), None),
        P(("expert", "dp"), None),
        P(("expert", "dp"), None),
        P("expert", "dp", None, None, None),
        P("expert", "dp", None),
    )
    return jax.shard_map(
        body,
        mesh=mesh,
        in_specs=placed,
        out_specs=(
            P("expert", "dp", None, None, None),
            P("expert", "dp", None),
            P(("expert", "dp"), None),
        ),
        check_vma=False,
    )
```

```python
import functools

import jax
import jax.numpy as jnp
from jax import lax
from jax.experimental import pallas as pl
from jax.experimental.pallas import tpu as pltpu
from jax.sharding import PartitionSpec as P

MESH = pl.DeviceIdType.MESH
PIECES = 8


def kernel(
    window, shards, capacity, pieces,
    token_hbm, logits_hbm, chosen_hbm, slots_hbm, other_hbm, hidden_hbm, weight_ref,
    gradh_ref, down_ref, logit_ref,
    token_ref, logits_ref, chosen_ref, slots_ref, other_ref, hidden_ref,
    rsend, rrecv, msend, mrecv, wfull, padded, hturn, upward, own, csend, crecv, ysend, yrecv,
    tsend, trecv, gates,
    rs, rr, ms, mr, ws, wr, fs, fr, cs, cr, ys, yr, ts, tr, ls, lw,
):
    me = lax.axis_index("expert")
    place = lax.axis_index("dp")
    chip, core = place // 2, place % 2
    chips = shards // 2
    mate = (me, chip * 2 + 1 - core)
    tokens, width = token_ref.shape
    piece = width // pieces
    rows = rsend.shape[2]
    slots_all = window * rows
    shard_rows, hidden_units = weight_ref.shape[0], hidden_ref.shape[2]

    def other(step):
        return lax.rem(me + step, window)

    def chip_at(step):
        return lax.rem(chip + step, chips)

    def across(step):
        return (me, chip_at(step) * 2 + core)

    loads = [
        pltpu.make_async_copy(src, dst, ls.at[i])
        for i, (src, dst) in enumerate((
            (chosen_hbm, chosen_ref), (slots_hbm, slots_ref), (token_hbm, token_ref),
            (logits_hbm, logits_ref), (other_hbm, other_ref), (hidden_hbm, hidden_ref),
        ))
    ]
    for load in loads:
        load.start()
    keeps = [
        pltpu.make_async_copy(
            weight_ref.at[:, pl.ds(c * piece, piece)], wfull.at[c, place], lw.at[c]
        )
        for c in range(pieces)
    ]

    def weight_copy(c, target, step, slot):
        lanes = pl.ds(pl.multiple_of(c * piece, piece), piece)
        return pltpu.make_async_remote_copy(
            src_ref=weight_ref.at[:, lanes], dst_ref=wfull.at[c, slot],
            send_sem=ws.at[c, step], recv_sem=wr.at[c, step],
            device_id=target, device_id_type=MESH,
        )

    barrier = pltpu.get_barrier_semaphore()
    for step in range(1, window):
        pl.semaphore_signal(barrier, inc=1, device_id=(other(step), place), device_id_type=MESH)
    for step in range(1, chips):
        pl.semaphore_signal(barrier, inc=1, device_id=across(step), device_id_type=MESH)
    pl.semaphore_signal(barrier, inc=1, device_id=mate, device_id_type=MESH)

    k = logit_ref.shape[0]
    pl.semaphore_wait(barrier, window - 1 + chips)

    def launch_weights(c, carry):
        for step in range(1, chips):
            weight_copy(c, across(step), step, place).start()
        weight_copy(c, mate, 0, place).start()
        return carry

    lax.fori_loop(0, pieces, launch_weights, 0)

    for load in loads[:5]:
        load.wait()
    raised = jnp.exp(logits_ref[...])
    gating = raised / jnp.sum(raised, axis=0, keepdims=True)
    sent_gate = gating.astype(jnp.bfloat16).astype(jnp.float32)
    chosen = chosen_ref[...]
    slots = slots_ref[...]
    outside = jnp.where(chosen >= window, other_ref[...], 0.0)
    live = slots < capacity
    for w in range(window):
        here = live & (chosen == w)
        pos = jnp.sum(jnp.where(here, slots.astype(jnp.float32) + 1.0, 0.0), axis=0, keepdims=True) - 1.0
        gate = jnp.sum(jnp.where(here, sent_gate, 0.0), axis=0, keepdims=True)
        line = lax.broadcasted_iota(jnp.int32, (8, tokens), 0)
        msend[w] = jnp.where(line == 0, pos, gate)

    slot_id = lax.broadcasted_iota(jnp.int32, (rows, tokens), 0).astype(jnp.float32)

    def spread(ref, w):
        return slot_id == ref[w, 0:1, :]

    dispatch = jnp.concatenate(
        [spread(msend, w).astype(jnp.float32) for w in range(window)], axis=0
    ).astype(jnp.bfloat16)

    def fill(c):
        lanes = pl.ds(pl.multiple_of(c * piece, piece), piece)
        placed = jnp.dot(dispatch, token_ref[:, lanes], preferred_element_type=jnp.float32)
        rsend[c] = placed.astype(jnp.bfloat16).reshape(window, rows, piece)

    def row_copy(c, dest, source):
        return pltpu.make_async_remote_copy(
            src_ref=rsend.at[c, dest, pl.ds(0, capacity)],
            dst_ref=rrecv.at[c, source, pl.ds(0, capacity)],
            send_sem=rs.at[c, dest], recv_sem=rr.at[c, source],
            device_id=(dest, place), device_id_type=MESH,
        )

    def meta_copy(dest, source):
        return pltpu.make_async_remote_copy(
            src_ref=msend.at[dest], dst_ref=mrecv.at[source],
            send_sem=ms.at[dest], recv_sem=mr.at[source],
            device_id=(dest, place), device_id_type=MESH,
        )

    def score_copy(dest, source):
        return pltpu.make_async_remote_copy(
            src_ref=tsend.at[dest], dst_ref=trecv.at[source],
            send_sem=ts.at[dest], recv_sem=tr.at[source],
            device_id=(dest, place), device_id_type=MESH,
        )

    def pass_copy(c, step, slot):
        return pltpu.make_async_remote_copy(
            src_ref=wfull.at[c, slot], dst_ref=wfull.at[c, slot],
            send_sem=fs.at[c, step], recv_sem=fr.at[c, step],
            device_id=mate, device_id_type=MESH,
        )

    def core_copy(c):
        return pltpu.make_async_remote_copy(
            src_ref=csend.at[c], dst_ref=crecv.at[c],
            send_sem=cs.at[c], recv_sem=cr.at[c],
            device_id=mate, device_id_type=MESH,
        )

    def sum_copy(c, step):
        return pltpu.make_async_remote_copy(
            src_ref=ysend.at[c, step], dst_ref=yrecv.at[c, step],
            send_sem=ys.at[c, step], recv_sem=yr.at[c, step],
            device_id=across(step), device_id_type=MESH,
        )

    fill(0)
    for step in range(1, window):
        meta_copy(other(step), me).start()

    def launch(c, carry):
        for step in range(1, window):
            row_copy(c, other(step), me).start()

        @pl.when(c + 1 < pieces)
        def _():
            fill(c + 1)

        return carry

    lax.fori_loop(0, pieces, launch, 0)

    mrecv[me] = msend[me]
    for c in range(pieces):
        rrecv[c, me, 0:capacity] = rsend[c, me, 0:capacity]
        if rows > capacity:
            rrecv[c, :, capacity:rows] = jnp.zeros((window, rows - capacity, piece), jnp.bfloat16)
        keeps[c].start()
    loads[5].wait()
    padded[:, 0:capacity] = hidden_ref[...]
    if rows > capacity:
        padded[:, capacity:rows] = jnp.zeros((window, rows - capacity, hidden_units), jnp.bfloat16)
    flat = padded[...].reshape(slots_all, hidden_units)
    hturn[...] = flat.T.reshape(shards, shard_rows, slots_all)
    upward[...] = jnp.zeros_like(upward)
    for keep in keeps:
        keep.wait()

    for step in range(1, window):
        meta_copy(other(step), lax.rem(me + window - step, window)).wait_recv()
    for s in range(window):
        gates[s] = jnp.sum(
            jnp.where(spread(mrecv, s), mrecv[s, 1:2, :], 0.0), axis=1, keepdims=True
        )

    def finish(c, carry):
        lanes = pl.ds(pl.multiple_of(c * piece, piece), piece)
        for step in range(1, chips):
            came = lax.rem(chip + chips - step, chips) * 2 + core
            weight_copy(c, across(step), step, came).wait_recv()
            pass_copy(c, step, came).start()
        for step in range(1, window):
            row_copy(c, other(step), lax.rem(me + window - step, window)).wait_recv()
        got = rrecv[c].reshape(slots_all, piece)
        scaled = (gates[...].reshape(slots_all, 1) * got.astype(jnp.float32)).astype(jnp.bfloat16)
        for h in range(chips):
            csend[c, h] = jnp.dot(
                hturn[2 * h + 1 - core], scaled, preferred_element_type=jnp.float32
            ).astype(jnp.bfloat16)
        core_copy(c).start()
        for h in range(chips):
            own[h] = jnp.dot(hturn[2 * h + core], scaled, preferred_element_type=jnp.float32)
        weight_copy(c, mate, 0, chip * 2 + 1 - core).wait_recv()
        for step in range(1, chips):
            came = lax.rem(chip + chips - step, chips) * 2 + 1 - core
            pass_copy(c, step, came).wait_recv()
        weights = wfull[c].reshape(hidden_units, piece)
        upward[...] += lax.dot_general(
            got, weights, (((1,), (1,)), ((), ())), preferred_element_type=jnp.float32
        )
        core_copy(c).wait_recv()
        for step in range(1, chips):
            to = chip_at(step)
            ysend[c, step] = (own[to] + crecv[c, to].astype(jnp.float32)).astype(jnp.bfloat16)
            sum_copy(c, step).start()
        down_ref[:, lanes] = own[chip] + crecv[c, chip].astype(jnp.float32)
        return carry

    lax.fori_loop(0, pieces, finish, 0)

    for s in range(window):
        up = upward[s * rows : (s + 1) * rows]
        score = jnp.sum(padded[s].astype(jnp.float32) * up, axis=1, keepdims=True)
        back = jnp.sum(jnp.where(spread(mrecv, s), score, 0.0), axis=0, keepdims=True)
        tsend[s] = jnp.broadcast_to(back, (8, tokens))
    for step in range(1, window):
        score_copy(other(step), me).start()
    trecv[me] = tsend[me]
    for s in range(window):
        up = upward[s * rows : s * rows + capacity]
        gradh_ref[s] = (gates[s, 0:capacity] * up).astype(jnp.bfloat16)

    for step in range(1, window):
        score_copy(other(step), lax.rem(me + window - step, window)).wait_recv()
    token_scores = jnp.zeros((k, tokens), jnp.float32)
    for w in range(window):
        token_scores = jnp.where(chosen == w, trecv[w], token_scores)
    scores_all = jnp.where(live, token_scores, outside)
    mean_score = jnp.sum(gating * scores_all, axis=0, keepdims=True)
    logit_ref[...] = gating * (scores_all - mean_score)

    def collect(c, carry):
        lanes = pl.ds(pl.multiple_of(c * piece, piece), piece)
        for step in range(1, chips):
            sum_copy(c, step).wait_recv()
            down_ref[:, lanes] += yrecv[c, step].astype(jnp.float32)
        return carry

    lax.fori_loop(0, pieces, collect, 0)

    def drain(c, carry):
        for step in range(1, window):
            row_copy(c, other(step), me).wait_send()
        for step in range(1, chips):
            weight_copy(c, across(step), step, place).wait_send()
            pass_copy(c, step, lax.rem(chip + chips - step, chips) * 2 + core).wait_send()
            sum_copy(c, step).wait_send()
        weight_copy(c, mate, 0, place).wait_send()
        core_copy(c).wait_send()
        return carry

    lax.fori_loop(0, pieces, drain, 0)
    for step in range(1, window):
        meta_copy(other(step), me).wait_send()
        score_copy(other(step), me).wait_send()


def write_out(a, b, c, a_out, b_out, c_out, sems):
    copies = [
        pltpu.make_async_copy(src, dst, sems.at[i])
        for i, (src, dst) in enumerate(((b, b_out), (a, a_out), (c, c_out)))
    ]
    for copy in copies:
        copy.start()
    for copy in copies:
        copy.wait()


def fused(grad_output, logits, chosen, slots, other_scores, hidden, down_weight):
    window = lax.axis_size("expert")
    shards = lax.axis_size("dp")
    capacity, hidden_units = hidden.shape[3], hidden.shape[4]
    tokens, width = grad_output.shape
    k = logits.shape[1]
    shard_rows = down_weight.shape[1]
    rows = -(-capacity // 16) * 16
    chips = shards // 2
    piece = width // PIECES
    vmem = pl.BlockSpec(memory_space=pltpu.VMEM)
    hbm = pl.BlockSpec(memory_space=pltpu.HBM)
    bf, f32, dma = jnp.bfloat16, jnp.float32, pltpu.SemaphoreType.DMA
    slots_all = window * rows
    gradh, down, turned = pl.pallas_call(
        functools.partial(kernel, window, shards, capacity, PIECES),
        out_shape=(
            jax.ShapeDtypeStruct((window, capacity, hidden_units), bf),
            jax.ShapeDtypeStruct((shard_rows, width), f32),
            jax.ShapeDtypeStruct((k, tokens), f32),
        ),
        in_specs=[hbm] * 7,
        out_specs=(vmem,) * 3,
        scratch_shapes=[
            pltpu.VMEM((tokens, width), bf),
            pltpu.VMEM((k, tokens), f32),
            pltpu.VMEM((k, tokens), jnp.int32),
            pltpu.VMEM((k, tokens), jnp.int32),
            pltpu.VMEM((k, tokens), f32),
            pltpu.VMEM((window, capacity, hidden_units), bf),
            pltpu.VMEM((PIECES, window, rows, piece), bf),
            pltpu.VMEM((PIECES, window, rows, piece), bf),
            pltpu.VMEM((window, 8, tokens), f32),
            pltpu.VMEM((window, 8, tokens), f32),
            pltpu.VMEM((PIECES, shards, shard_rows, piece), bf),
            pltpu.VMEM((window, rows, hidden_units), bf),
            pltpu.VMEM((shards, shard_rows, slots_all), bf),
            pltpu.VMEM((slots_all, hidden_units), f32),
            pltpu.VMEM((chips, shard_rows, piece), f32),
            pltpu.VMEM((PIECES, chips, shard_rows, piece), bf),
            pltpu.VMEM((PIECES, chips, shard_rows, piece), bf),
            pltpu.VMEM((PIECES, chips, shard_rows, piece), bf),
            pltpu.VMEM((PIECES, chips, shard_rows, piece), bf),
            pltpu.VMEM((window, 8, tokens), f32),
            pltpu.VMEM((window, 8, tokens), f32),
            pltpu.VMEM((window, rows, 1), f32),
            dma((PIECES, window)), dma((PIECES, window)),
            dma((window,)), dma((window,)),
            dma((PIECES, chips)), dma((PIECES, chips)),
            dma((PIECES, chips)), dma((PIECES, chips)),
            dma((PIECES,)), dma((PIECES,)),
            dma((PIECES, chips)), dma((PIECES, chips)),
            dma((window,)), dma((window,)),
            dma((6,)), dma((PIECES,)),
        ],
        compiler_params=pltpu.CompilerParams(
            collective_id=0, has_side_effects=True, vmem_limit_bytes=48 * 1024 * 1024
        ),
    )(*(pltpu.with_memory_space_constraint(a, pltpu.HBM) for a in (
        grad_output, logits.T, chosen.T, slots.T, other_scores.T,
        hidden.reshape(window, capacity, hidden_units), down_weight.reshape(shard_rows, width),
    )))
    gradh, down, turned = (
        pltpu.with_memory_space_constraint(a, pltpu.VMEM) for a in (gradh, down, turned)
    )
    gradh, down, turned = pl.pallas_call(
        write_out,
        out_shape=tuple(jax.ShapeDtypeStruct(a.shape, a.dtype) for a in (gradh, down, turned)),
        in_specs=[vmem] * 3,
        out_specs=(hbm,) * 3,
        scratch_shapes=[dma((3,))],
        compiler_params=pltpu.CompilerParams(vmem_limit_bytes=8 * 1024 * 1024),
    )(gradh, down, turned)
    return (gradh.reshape(hidden.shape), down.reshape(1, shard_rows, width), turned.T)


def plain(grad_output, logits, chosen, slots, other_scores, hidden, down_weight):
    window = lax.axis_size("expert")
    capacity = hidden.shape[3]
    hidden_units = hidden.shape[4]
    model_width = grad_output.shape[1]
    shard_rows = down_weight.shape[1]
    raised = jnp.exp(logits)
    gating = raised / jnp.sum(raised, axis=1, keepdims=True)
    gate_sent = gating.astype(jnp.bfloat16)
    live_slot = slots < capacity
    target = jnp.where(live_slot, chosen * capacity + slots, window * capacity)
    columns = jnp.arange(window * capacity, dtype=jnp.int32)
    placing = (target[:, :, None] == columns[None, None, :]).astype(jnp.bfloat16)
    dispatch = jnp.sum(placing, axis=1)
    send_rows = jnp.einsum(
        "tr,td->rd", dispatch, grad_output, preferred_element_type=jnp.float32
    ).astype(jnp.bfloat16)
    send_gate = jnp.einsum(
        "tkr,tk->r", placing, gate_sent, preferred_element_type=jnp.float32
    ).astype(jnp.bfloat16)
    placing_float = placing.astype(jnp.float32)
    send_rows = send_rows.reshape(window, capacity, model_width)
    send_gate = send_gate.reshape(window, capacity)
    recv_rows, recv_gate = (
        lax.all_to_all(send_rows, "expert", split_axis=0, concat_axis=0, tiled=True),
        lax.all_to_all(send_gate, "expert", split_axis=0, concat_axis=0, tiled=True),
    )
    slot_rows = recv_rows.reshape(-1, model_width)
    slot_gate = recv_gate.reshape(-1).astype(jnp.float32)
    local_hidden = hidden.reshape(-1, hidden_units)
    scaled = (slot_gate[:, None] * slot_rows.astype(jnp.float32)).astype(jnp.bfloat16)
    weights = down_weight.reshape(shard_rows, model_width)
    product = lax.dot_general(
        slot_rows,
        lax.all_gather(weights, "dp", axis=0, tiled=True),
        (((1,), (1,)), ((), ())),
        preferred_element_type=jnp.float32,
    )
    grad_rows = lax.psum_scatter(
        lax.dot_general(
            local_hidden, scaled, (((0,), (0,)), ((), ())), preferred_element_type=jnp.float32
        ).astype(jnp.bfloat16),
        "dp",
        scatter_dimension=0,
        tiled=True,
    ).astype(jnp.float32)
    slot_scores = jnp.sum(local_hidden.astype(jnp.float32) * product, axis=1)
    grad_hidden = (slot_gate[:, None] * product).astype(jnp.bfloat16).reshape(hidden.shape)
    returned = lax.all_to_all(
        slot_scores.reshape(window, capacity), "expert", split_axis=0, concat_axis=0, tiled=True
    )
    token_scores = jnp.einsum(
        "tkr,r->tk", placing_float, returned.reshape(-1), precision=lax.Precision.HIGHEST
    )
    outside = jnp.where(chosen >= window, other_scores, jnp.float32(0.0))
    scores_all = jnp.where(live_slot, token_scores, outside)
    mean_score = jnp.sum(gating * scores_all, axis=1, keepdims=True)
    grad_logits = gating * (scores_all - mean_score)
    return (grad_hidden, grad_rows.reshape(1, shard_rows, model_width), grad_logits)


def body(grad_output, logits, chosen, slots, other_scores, hidden, down_weight):
    args = (grad_output, logits, chosen, slots, other_scores, hidden, down_weight)
    fits = (
        lax.axis_size("dp") % 2 == 0
        and hidden.shape[3] % 8 == 0
        and down_weight.shape[1] % 16 == 0
        and hidden.shape[4] % 128 == 0
        and grad_output.shape[0] == 128
        and grad_output.shape[1] % (PIECES * 128) == 0
        and logits.shape[1] == 8
    )
    return fused(*args) if fits else plain(*args)


def solution(mesh):
    placed = (
        P(("expert", "dp"), None),
        P(("expert", "dp"), None),
        P(("expert", "dp"), None),
        P(("expert", "dp"), None),
        P(("expert", "dp"), None),
        P("expert", "dp", None, None, None),
        P("expert", "dp", None),
    )
    return jax.shard_map(
        body,
        mesh=mesh,
        in_specs=placed,
        out_specs=(
            P("expert", "dp", None, None, None),
            P("expert", "dp", None),
            P(("expert", "dp"), None),
        ),
        check_vma=False,
    )
```

```python
import functools

import jax
import jax.numpy as jnp
from jax import lax
from jax.experimental import pallas as pl
from jax.experimental.pallas import tpu as pltpu
from jax.sharding import PartitionSpec as P

MESH = pl.DeviceIdType.MESH
PIECES = 8


def kernel(
    window, shards, capacity, pieces,
    token_hbm, logits_hbm, chosen_hbm, slots_hbm, other_hbm, hidden_hbm, weight_ref,
    gradh_ref, down_ref, logit_ref,
    token_ref, logits_ref, chosen_ref, slots_ref, other_ref, hidden_ref,
    rsend, rrecv, msend, mrecv, wfull, padded, hturn, upward, own, csend, crecv, ysend, yrecv,
    tsend, trecv, gates,
    rs, rr, ms, mr, ws, wr, fs, fr, cs, cr, ys, yr, ts, tr, ls, lw,
):
    me = lax.axis_index("expert")
    place = lax.axis_index("dp")
    chip, core = place // 2, place % 2
    chips = shards // 2
    mate = (me, chip * 2 + 1 - core)
    tokens, width = token_ref.shape
    piece = width // pieces
    rows = rsend.shape[2]
    slots_all = window * rows
    shard_rows, hidden_units = weight_ref.shape[0], hidden_ref.shape[2]

    near = [lax.rem(me + step, window) for step in range(window)]

    def other(step):
        return near[step]

    def settle(buffer, sem):
        whole = buffer.at[pl.ds(0, window - 1)]
        pltpu.make_async_copy(whole, whole, sem).wait()

    def chip_at(step):
        return lax.rem(chip + step, chips)

    def across(step):
        return (me, chip_at(step) * 2 + core)

    loads = [
        pltpu.make_async_copy(src, dst, ls.at[i])
        for i, (src, dst) in enumerate((
            (chosen_hbm, chosen_ref), (slots_hbm, slots_ref), (token_hbm, token_ref),
            (logits_hbm, logits_ref), (other_hbm, other_ref), (hidden_hbm, hidden_ref),
        ))
    ]
    for load in loads:
        load.start()
    keeps = [
        pltpu.make_async_copy(
            weight_ref.at[:, pl.ds(c * piece, piece)], wfull.at[c, place], lw.at[c]
        )
        for c in range(pieces)
    ]

    def weight_copy(c, target, step, slot):
        lanes = pl.ds(pl.multiple_of(c * piece, piece), piece)
        return pltpu.make_async_remote_copy(
            src_ref=weight_ref.at[:, lanes], dst_ref=wfull.at[c, slot],
            send_sem=ws.at[c, step], recv_sem=wr.at[c, step],
            device_id=target, device_id_type=MESH,
        )

    barrier = pltpu.get_barrier_semaphore()
    for step in range(1, window):
        pl.semaphore_signal(barrier, inc=1, device_id=(other(step), place), device_id_type=MESH)
    for step in range(1, chips):
        pl.semaphore_signal(barrier, inc=1, device_id=across(step), device_id_type=MESH)
    pl.semaphore_signal(barrier, inc=1, device_id=mate, device_id_type=MESH)

    k = logit_ref.shape[0]
    for load in loads[:5]:
        load.wait()
    raised = jnp.exp(logits_ref[...])
    gating = raised / jnp.sum(raised, axis=0, keepdims=True)
    sent_gate = gating.astype(jnp.bfloat16).astype(jnp.float32)
    chosen = chosen_ref[...]
    slots = slots_ref[...]
    outside = jnp.where(chosen >= window, other_ref[...], 0.0)
    live = slots < capacity
    for w in range(window):
        here = live & (chosen == w)
        pos = jnp.sum(jnp.where(here, slots.astype(jnp.float32) + 1.0, 0.0), axis=0, keepdims=True) - 1.0
        gate = jnp.sum(jnp.where(here, sent_gate, 0.0), axis=0, keepdims=True)
        line = lax.broadcasted_iota(jnp.int32, (8, tokens), 0)
        msend[w] = jnp.where(line == 0, pos, gate)

    slot_id = lax.broadcasted_iota(jnp.int32, (rows, tokens), 0).astype(jnp.float32)

    def spread(ref, w):
        return slot_id == ref[w, 0:1, :]

    dispatch = jnp.concatenate(
        [spread(msend, w).astype(jnp.float32) for w in range(window)], axis=0
    ).astype(jnp.bfloat16)

    def fill(c):
        lanes = pl.ds(pl.multiple_of(c * piece, piece), piece)
        placed = jnp.dot(dispatch, token_ref[:, lanes], preferred_element_type=jnp.float32)
        rsend[c] = placed.astype(jnp.bfloat16).reshape(window, rows, piece)

    def row_copy(c, dest, source):
        return pltpu.make_async_remote_copy(
            src_ref=rsend.at[c, dest, pl.ds(0, capacity)],
            dst_ref=rrecv.at[c, source, pl.ds(0, capacity)],
            send_sem=rs, recv_sem=rr.at[c],
            device_id=(dest, place), device_id_type=MESH,
        )

    def meta_copy(dest, source):
        return pltpu.make_async_remote_copy(
            src_ref=msend.at[dest], dst_ref=mrecv.at[source],
            send_sem=ms, recv_sem=mr,
            device_id=(dest, place), device_id_type=MESH,
        )

    def score_copy(dest, source):
        return pltpu.make_async_remote_copy(
            src_ref=tsend.at[dest], dst_ref=trecv.at[source],
            send_sem=ts, recv_sem=tr,
            device_id=(dest, place), device_id_type=MESH,
        )

    def pass_copy(c, step, slot):
        return pltpu.make_async_remote_copy(
            src_ref=wfull.at[c, slot], dst_ref=wfull.at[c, slot],
            send_sem=fs.at[c, step], recv_sem=fr.at[c, step],
            device_id=mate, device_id_type=MESH,
        )

    def core_copy(c):
        return pltpu.make_async_remote_copy(
            src_ref=csend.at[c], dst_ref=crecv.at[c],
            send_sem=cs.at[c], recv_sem=cr.at[c],
            device_id=mate, device_id_type=MESH,
        )

    def sum_copy(c, step):
        return pltpu.make_async_remote_copy(
            src_ref=ysend.at[c, step], dst_ref=yrecv.at[c, step],
            send_sem=ys.at[c, step], recv_sem=yr.at[c, step],
            device_id=across(step), device_id_type=MESH,
        )

    fill(0)
    pl.semaphore_wait(barrier, window - 1 + chips)

    def launch_weights(c, carry):
        for step in range(1, chips):
            weight_copy(c, across(step), step, place).start()
        weight_copy(c, mate, 0, place).start()
        return carry

    lax.fori_loop(0, pieces, launch_weights, 0)

    for step in range(1, window):
        meta_copy(other(step), me).start()

    def launch(c, carry):
        for step in range(1, window):
            row_copy(c, other(step), me).start()

        @pl.when(c + 1 < pieces)
        def _():
            fill(c + 1)

        return carry

    lax.fori_loop(0, pieces, launch, 0)

    mrecv[me] = msend[me]
    for c in range(pieces):
        rrecv[c, me, 0:capacity] = rsend[c, me, 0:capacity]
        if rows > capacity:
            rrecv[c, :, capacity:rows] = jnp.zeros((window, rows - capacity, piece), jnp.bfloat16)
        keeps[c].start()
    loads[5].wait()
    padded[:, 0:capacity] = hidden_ref[...]
    if rows > capacity:
        padded[:, capacity:rows] = jnp.zeros((window, rows - capacity, hidden_units), jnp.bfloat16)
    flat = padded[...].reshape(slots_all, hidden_units)
    hturn[...] = flat.T.reshape(shards, shard_rows, slots_all)
    upward[...] = jnp.zeros_like(upward)
    for keep in keeps:
        keep.wait()

    settle(mrecv, mr)
    for s in range(window):
        gates[s] = jnp.sum(
            jnp.where(spread(mrecv, s), mrecv[s, 1:2, :], 0.0), axis=1, keepdims=True
        )

    def combine(c):
        lanes = pl.ds(pl.multiple_of(c * piece, piece), piece)
        core_copy(c).wait_recv()
        for step in range(1, chips):
            to = chip_at(step)
            ysend[c, step] = (own[c, to] + crecv[c, to].astype(jnp.float32)).astype(jnp.bfloat16)
            sum_copy(c, step).start()
        down_ref[:, lanes] = own[c, chip] + crecv[c, chip].astype(jnp.float32)

    def finish(c, carry):
        for step in range(1, chips):
            came = lax.rem(chip + chips - step, chips) * 2 + core
            weight_copy(c, across(step), step, came).wait_recv()
            pass_copy(c, step, came).start()
        came_rows = rrecv.at[c, pl.ds(0, window - 1), pl.ds(0, capacity)]
        pltpu.make_async_copy(came_rows, came_rows, rr.at[c]).wait()
        got = rrecv[c].reshape(slots_all, piece)
        scaled = (gates[...].reshape(slots_all, 1) * got.astype(jnp.float32)).astype(jnp.bfloat16)
        for h in range(chips):
            csend[c, h] = jnp.dot(
                hturn[2 * h + 1 - core], scaled, preferred_element_type=jnp.float32
            ).astype(jnp.bfloat16)
        core_copy(c).start()
        for h in range(chips):
            own[c, h] = jnp.dot(hturn[2 * h + core], scaled, preferred_element_type=jnp.float32)
        weight_copy(c, mate, 0, chip * 2 + 1 - core).wait_recv()
        for step in range(1, chips):
            came = lax.rem(chip + chips - step, chips) * 2 + 1 - core
            pass_copy(c, step, came).wait_recv()
        weights = wfull[c].reshape(hidden_units, piece)
        upward[...] += lax.dot_general(
            got, weights, (((1,), (1,)), ((), ())), preferred_element_type=jnp.float32
        )

        @pl.when(c > 0)
        def _():
            combine(c - 1)

        return carry

    lax.fori_loop(0, pieces, finish, 0)
    combine(pieces - 1)

    for s in range(window):
        up = upward[s * rows : (s + 1) * rows]
        score = jnp.sum(padded[s].astype(jnp.float32) * up, axis=1, keepdims=True)
        back = jnp.sum(jnp.where(spread(mrecv, s), score, 0.0), axis=0, keepdims=True)
        tsend[s] = jnp.broadcast_to(back, (8, tokens))
    for step in range(1, window):
        score_copy(other(step), me).start()
    trecv[me] = tsend[me]
    for s in range(window):
        up = upward[s * rows : s * rows + capacity]
        gradh_ref[s] = (gates[s, 0:capacity] * up).astype(jnp.bfloat16)

    def collect(c, carry):
        lanes = pl.ds(pl.multiple_of(c * piece, piece), piece)
        for step in range(1, chips):
            sum_copy(c, step).wait_recv()
            down_ref[:, lanes] += yrecv[c, step].astype(jnp.float32)
        return carry

    def drain(c, carry):
        for step in range(1, chips):
            weight_copy(c, across(step), step, place).wait_send()
            pass_copy(c, step, lax.rem(chip + chips - step, chips) * 2 + core).wait_send()
        weight_copy(c, mate, 0, place).wait_send()
        core_copy(c).wait_send()
        return carry

    lax.fori_loop(0, pieces, drain, 0)
    sent_rows = rsend.at[:, pl.ds(0, window - 1), pl.ds(0, capacity)]
    pltpu.make_async_copy(sent_rows, sent_rows, rs).wait()
    settle(msend, ms)
    lax.fori_loop(0, pieces - 1, collect, 0)

    settle(trecv, tr)
    token_scores = jnp.zeros((k, tokens), jnp.float32)
    for w in range(window):
        token_scores = jnp.where(chosen == w, trecv[w], token_scores)
    scores_all = jnp.where(live, token_scores, outside)
    mean_score = jnp.sum(gating * scores_all, axis=0, keepdims=True)
    logit_ref[...] = gating * (scores_all - mean_score)
    settle(tsend, ts)

    collect(pieces - 1, 0)
    for c in range(pieces):
        for step in range(1, chips):
            sum_copy(c, step).wait_send()


def write_out(a, b, c, a_out, b_out, c_out, sems):
    copies = [
        pltpu.make_async_copy(src, dst, sems.at[i])
        for i, (src, dst) in enumerate(((b, b_out), (a, a_out), (c, c_out)))
    ]
    for copy in copies:
        copy.start()
    for copy in copies:
        copy.wait()


def fused(grad_output, logits, chosen, slots, other_scores, hidden, down_weight):
    window = lax.axis_size("expert")
    shards = lax.axis_size("dp")
    capacity, hidden_units = hidden.shape[3], hidden.shape[4]
    tokens, width = grad_output.shape
    k = logits.shape[1]
    shard_rows = down_weight.shape[1]
    rows = -(-capacity // 16) * 16
    chips = shards // 2
    piece = width // PIECES
    vmem = pl.BlockSpec(memory_space=pltpu.VMEM)
    hbm = pl.BlockSpec(memory_space=pltpu.HBM)
    bf, f32, dma = jnp.bfloat16, jnp.float32, pltpu.SemaphoreType.DMA
    slots_all = window * rows
    gradh, down, turned = pl.pallas_call(
        functools.partial(kernel, window, shards, capacity, PIECES),
        out_shape=(
            jax.ShapeDtypeStruct((window, capacity, hidden_units), bf),
            jax.ShapeDtypeStruct((shard_rows, width), f32),
            jax.ShapeDtypeStruct((k, tokens), f32),
        ),
        in_specs=[hbm] * 7,
        out_specs=(vmem,) * 3,
        scratch_shapes=[
            pltpu.VMEM((tokens, width), bf),
            pltpu.VMEM((k, tokens), f32),
            pltpu.VMEM((k, tokens), jnp.int32),
            pltpu.VMEM((k, tokens), jnp.int32),
            pltpu.VMEM((k, tokens), f32),
            pltpu.VMEM((window, capacity, hidden_units), bf),
            pltpu.VMEM((PIECES, window, rows, piece), bf),
            pltpu.VMEM((PIECES, window, rows, piece), bf),
            pltpu.VMEM((window, 8, tokens), f32),
            pltpu.VMEM((window, 8, tokens), f32),
            pltpu.VMEM((PIECES, shards, shard_rows, piece), bf),
            pltpu.VMEM((window, rows, hidden_units), bf),
            pltpu.VMEM((shards, shard_rows, slots_all), bf),
            pltpu.VMEM((slots_all, hidden_units), f32),
            pltpu.VMEM((PIECES, chips, shard_rows, piece), f32),
            pltpu.VMEM((PIECES, chips, shard_rows, piece), bf),
            pltpu.VMEM((PIECES, chips, shard_rows, piece), bf),
            pltpu.VMEM((PIECES, chips, shard_rows, piece), bf),
            pltpu.VMEM((PIECES, chips, shard_rows, piece), bf),
            pltpu.VMEM((window, 8, tokens), f32),
            pltpu.VMEM((window, 8, tokens), f32),
            pltpu.VMEM((window, rows, 1), f32),
            dma, dma((PIECES,)),
            dma, dma,
            dma((PIECES, chips)), dma((PIECES, chips)),
            dma((PIECES, chips)), dma((PIECES, chips)),
            dma((PIECES,)), dma((PIECES,)),
            dma((PIECES, chips)), dma((PIECES, chips)),
            dma, dma,
            dma((6,)), dma((PIECES,)),
        ],
        compiler_params=pltpu.CompilerParams(
            collective_id=0, has_side_effects=True, vmem_limit_bytes=48 * 1024 * 1024
        ),
    )(*(pltpu.with_memory_space_constraint(a, pltpu.HBM) for a in (
        grad_output, logits.T, chosen.T, slots.T, other_scores.T,
        hidden.reshape(window, capacity, hidden_units), down_weight.reshape(shard_rows, width),
    )))
    gradh, down, turned = (
        pltpu.with_memory_space_constraint(a, pltpu.VMEM) for a in (gradh, down, turned)
    )
    gradh, down, turned = pl.pallas_call(
        write_out,
        out_shape=tuple(jax.ShapeDtypeStruct(a.shape, a.dtype) for a in (gradh, down, turned)),
        in_specs=[vmem] * 3,
        out_specs=(hbm,) * 3,
        scratch_shapes=[dma((3,))],
        compiler_params=pltpu.CompilerParams(vmem_limit_bytes=8 * 1024 * 1024),
    )(gradh, down, turned)
    return (gradh.reshape(hidden.shape), down.reshape(1, shard_rows, width), turned.T)


def plain(grad_output, logits, chosen, slots, other_scores, hidden, down_weight):
    window = lax.axis_size("expert")
    capacity = hidden.shape[3]
    hidden_units = hidden.shape[4]
    model_width = grad_output.shape[1]
    shard_rows = down_weight.shape[1]
    raised = jnp.exp(logits)
    gating = raised / jnp.sum(raised, axis=1, keepdims=True)
    gate_sent = gating.astype(jnp.bfloat16)
    live_slot = slots < capacity
    target = jnp.where(live_slot, chosen * capacity + slots, window * capacity)
    columns = jnp.arange(window * capacity, dtype=jnp.int32)
    placing = (target[:, :, None] == columns[None, None, :]).astype(jnp.bfloat16)
    dispatch = jnp.sum(placing, axis=1)
    send_rows = jnp.einsum(
        "tr,td->rd", dispatch, grad_output, preferred_element_type=jnp.float32
    ).astype(jnp.bfloat16)
    send_gate = jnp.einsum(
        "tkr,tk->r", placing, gate_sent, preferred_element_type=jnp.float32
    ).astype(jnp.bfloat16)
    placing_float = placing.astype(jnp.float32)
    send_rows = send_rows.reshape(window, capacity, model_width)
    send_gate = send_gate.reshape(window, capacity)
    recv_rows, recv_gate = (
        lax.all_to_all(send_rows, "expert", split_axis=0, concat_axis=0, tiled=True),
        lax.all_to_all(send_gate, "expert", split_axis=0, concat_axis=0, tiled=True),
    )
    slot_rows = recv_rows.reshape(-1, model_width)
    slot_gate = recv_gate.reshape(-1).astype(jnp.float32)
    local_hidden = hidden.reshape(-1, hidden_units)
    scaled = (slot_gate[:, None] * slot_rows.astype(jnp.float32)).astype(jnp.bfloat16)
    weights = down_weight.reshape(shard_rows, model_width)
    product = lax.dot_general(
        slot_rows,
        lax.all_gather(weights, "dp", axis=0, tiled=True),
        (((1,), (1,)), ((), ())),
        preferred_element_type=jnp.float32,
    )
    grad_rows = lax.psum_scatter(
        lax.dot_general(
            local_hidden, scaled, (((0,), (0,)), ((), ())), preferred_element_type=jnp.float32
        ).astype(jnp.bfloat16),
        "dp",
        scatter_dimension=0,
        tiled=True,
    ).astype(jnp.float32)
    slot_scores = jnp.sum(local_hidden.astype(jnp.float32) * product, axis=1)
    grad_hidden = (slot_gate[:, None] * product).astype(jnp.bfloat16).reshape(hidden.shape)
    returned = lax.all_to_all(
        slot_scores.reshape(window, capacity), "expert", split_axis=0, concat_axis=0, tiled=True
    )
    token_scores = jnp.einsum(
        "tkr,r->tk", placing_float, returned.reshape(-1), precision=lax.Precision.HIGHEST
    )
    outside = jnp.where(chosen >= window, other_scores, jnp.float32(0.0))
    scores_all = jnp.where(live_slot, token_scores, outside)
    mean_score = jnp.sum(gating * scores_all, axis=1, keepdims=True)
    grad_logits = gating * (scores_all - mean_score)
    return (grad_hidden, grad_rows.reshape(1, shard_rows, model_width), grad_logits)


def body(grad_output, logits, chosen, slots, other_scores, hidden, down_weight):
    args = (grad_output, logits, chosen, slots, other_scores, hidden, down_weight)
    fits = (
        lax.axis_size("dp") % 2 == 0
        and hidden.shape[3] % 8 == 0
        and down_weight.shape[1] % 16 == 0
        and hidden.shape[4] % 128 == 0
        and grad_output.shape[0] == 128
        and grad_output.shape[1] % (PIECES * 128) == 0
        and logits.shape[1] == 8
    )
    return fused(*args) if fits else plain(*args)


def solution(mesh):
    placed = (
        P(("expert", "dp"), None),
        P(("expert", "dp"), None),
        P(("expert", "dp"), None),
        P(("expert", "dp"), None),
        P(("expert", "dp"), None),
        P("expert", "dp", None, None, None),
        P("expert", "dp", None),
    )
    return jax.shard_map(
        body,
        mesh=mesh,
        in_specs=placed,
        out_specs=(
            P("expert", "dp", None, None, None),
            P("expert", "dp", None),
            P(("expert", "dp"), None),
        ),
        check_vma=False,
    )
```
